128 devices in a mesh: wide: 32 (over x, z, core), narrow: 4 (over y).
Axes of the slice: x: 4, y: 4, z: 4, core: 2. Of those that a mesh axis runs over, the one named last changes fastest.
Arguments:
- table: bfloat16 [131072, 512], P(('wide', 'narrow')), may hold values from -1.5 to 1.5
- relations: bfloat16 [7424, 512], replicated, may hold values from -6 to 6
- req_rows: int32 [128, 2048], P(('wide', 'narrow')), may hold values from 0 to 1023, as said below
- owner_count: int32 [128, 128], P(('wide', 'narrow')), may hold values from 1 to 16, as said below
- owner_start: int32 [128, 128], P(('wide', 'narrow')), may hold values from 0 to 2032, as said below
- head_slot: int32 [131072], P(('wide', 'narrow')), may hold values from 0 to 2047, as said below
- rel_id: int32 [131072], P(('wide', 'narrow')), may hold values from 0 to 7423
- tail_slot: int32 [131072], P(('wide', 'narrow')), may hold values from 0 to 2047, as said below
- neg_slot: int32 [131072], P(('wide', 'narrow')), may hold values from 0 to 2047, as said below
Outputs:
- table_grad: float32 [131072, 512], P(('wide', 'narrow'))
The draws below stay inside these ranges and needn't reach their ends.
Inputs may be any that keep to these rules, and one draw needn't show every extreme that they name: `req_rows`: entries past the device's total of owner_count are ignored. A row may be asked more than once by one device of one owner; the gradients of all its slots add. `owner_count`: in every draw some owners receive exactly 16 rows from every device, and some device asks 16 rows of every owner. `owner_start`: the running sum of owner_count along owners, starting at 0. `head_slot`: below the device's total of owner_count. `tail_slot`: below the device's total of owner_count. `neg_slot`: below the device's total of owner_count.
All inputs are finite; a program needn't handle non-finite values.
Results may differ from the reference program's by a relative error of at most 0.0065.
Values may be sent and summed in bfloat16 or wider, within the bound.
A program may use at most 64 MiB of HBM per device.

```python
import math
import jax
import jax.numpy as jnp
import numpy as np
from jax import lax

D = 512
NREL = 7424
ENT_DEV = 1024
B_DEV = 1024
NEG = 1024
CAP = 16
OWNERS = 128
SLOTS = 2048
ENTITIES = 131072


def layout(key):
    base = jax.random.fold_in(key, 7001)
    hot = jax.random.randint(jax.random.fold_in(base, 1), (4,), 0, OWNERS)
    counts = jax.random.randint(jax.random.fold_in(base, 2), (OWNERS, OWNERS), 1, CAP // 2 + 1)
    is_hot = jnp.any(jnp.arange(OWNERS)[:, None] == hot[None, :], axis=1)
    counts = jnp.where(is_hot[None, :], CAP, counts)
    filled = jax.random.randint(jax.random.fold_in(base, 3), (), 0, OWNERS)
    is_full = jnp.arange(OWNERS)[:, None] == filled
    counts = jnp.where(is_full, CAP, counts).astype(jnp.int32)
    starts = (jnp.cumsum(counts, axis=1) - counts).astype(jnp.int32)
    totals = jnp.sum(counts, axis=1).astype(jnp.int32)
    return (counts, starts, totals)


def draw_req_rows(key, part):
    return jax.random.randint(jax.random.fold_in(key, 7101), (OWNERS, SLOTS), 0, ENT_DEV).astype(jnp.int32)


def draw_owner_count(key, part):
    return layout(key)[0]


def draw_owner_start(key, part):
    return layout(key)[1]


def draw_slots(key, salt, width):
    totals = layout(key)[2]
    picks = jax.random.randint(jax.random.fold_in(key, salt), (OWNERS, width), 0, totals[:, None])
    places = jax.random.randint(jax.random.fold_in(key, salt + 50), (OWNERS, 1), 0, width)
    column = jnp.arange(width)[None, :]
    picks = jnp.where(column == places, totals[:, None] - 1, picks)
    return picks.reshape(-1).astype(jnp.int32)


def draw_head_slot(key, part):
    return draw_slots(key, 7201, B_DEV)


def draw_tail_slot(key, part):
    return draw_slots(key, 7202, B_DEV)


def draw_neg_slot(key, part):
    return draw_slots(key, 7203, NEG)


def touch_ends(values, key, smallest, largest):
    longest = values.shape.index(max(values.shape))
    spots = []
    for shift in (0, 1):
        where = [jax.random.randint(jax.random.fold_in(key, axis), (), 0, length) for axis, length in enumerate(values.shape)]
        where[longest] = (where[longest] + shift) % values.shape[longest]
        spots.append(tuple(where))
    return values.at[spots[0]].set(smallest).at[spots[1]].set(largest)


def steps_of(key, shape, split, low, high):
    def one(axis_at, blocks):
        steps = jax.random.uniform(jax.random.fold_in(jax.random.fold_in(key, 6), axis_at), (blocks,), jnp.float32, low / len(split), high / len(split))
        return jnp.repeat(jnp.exp(steps), shape[axis_at] // blocks).reshape((-1,) + (1,) * (len(shape) - axis_at - 1))

    factor_of = one(*split[0])
    for cut in split[1:]:
        factor_of = factor_of * one(*cut)
    return factor_of


def rank_table(number_of, lean):
    loads = [(1 << 20) // math.isqrt(standing ** lean) + 1 for standing in range(1, number_of + 1)]
    deviation = 1 + sum(loads) // (1 << 30)
    return np.cumsum(np.array([max(1, weight // deviation) for weight in loads]))


def ranked(own_key, shape, amount, lean):
    grid = rank_table(amount, lean)
    lot = jax.random.randint(jax.random.fold_in(own_key, 1), shape, 0, int(grid[amount - 1]))
    standing = jnp.searchsorted(jnp.asarray(grid, jnp.int32), lot, side="right")
    return jax.random.permutation(jax.random.fold_in(own_key, 2), amount)[standing].astype(jnp.int32)


def scatter_about(own_key, dims, deviation, reach, pieces=(), held_as=jnp.bfloat16):
    gain = steps_of(own_key, dims, pieces, -0.22, 0.18) if pieces else 1.0
    result = jax.random.normal(own_key, dims, jnp.float32) * deviation * gain
    return jnp.minimum(jnp.maximum(result, -reach), reach).astype(held_as)


def setup_inputs(seed: int = 0) -> dict:
    seeds = jax.random.split(jax.random.key(seed), 10)
    return {
        "table": scatter_about(seeds[0], (ENTITIES, D), 0.25, 1.5, ((0, 128),)),
        "relations": scatter_about(seeds[1], (NREL, D), 1.0, 6.0),
        "req_rows": draw_req_rows(jax.random.fold_in(seeds[9], 71), 0),
        "owner_count": draw_owner_count(jax.random.fold_in(seeds[9], 71), 0),
        "owner_start": draw_owner_start(jax.random.fold_in(seeds[9], 71), 0),
        "head_slot": draw_head_slot(jax.random.fold_in(seeds[9], 71), 0),
        "rel_id": touch_ends(ranked(seeds[6], (OWNERS * B_DEV,), NREL, 2), jax.random.fold_in(seeds[6], 3), 0, NREL - 1).astype(jnp.int32),
        "tail_slot": draw_tail_slot(jax.random.fold_in(seeds[9], 71), 0),
        "neg_slot": draw_neg_slot(jax.random.fold_in(seeds[9], 71), 0),
    }


def locate(slot_ids, start, count, cap):
    owners = start.shape[0]
    offset = slot_ids[:, None] - start[None, :]
    match = (offset >= 0) & (offset < count[None, :])
    owner_ids = jnp.arange(owners, dtype=jnp.int32)
    flat = jnp.sum(jnp.where(match, owner_ids[None, :] * cap + offset, 0), axis=1).astype(jnp.int32)
    valid = jnp.any(match, axis=1)
    return flat, valid


def slot_gradients(rows, flat, valid, rel_rows, batch):
    emb = jnp.where(valid[:, None], jnp.take(rows, flat, axis=0), jnp.zeros((), jnp.bfloat16))
    head = emb[:batch]
    tail = emb[batch:2 * batch]
    negative = emb[2 * batch:]
    rvec = rel_rows.astype(jnp.float32)
    query = head.astype(jnp.float32) * rvec
    query_half = query.astype(jnp.bfloat16)
    positive = jnp.sum(query * tail.astype(jnp.float32), axis=1)
    negative_score = lax.dot_general(query_half, negative, (((1,), (1,)), ((), ())), preferred_element_type=jnp.float32)
    pos_weight = -jax.nn.sigmoid(-positive)
    neg_weight = jax.nn.sigmoid(negative_score).astype(jnp.bfloat16)
    head_grad = rvec * (pos_weight[:, None] * tail.astype(jnp.float32) + jnp.dot(neg_weight, negative, preferred_element_type=jnp.float32))
    tail_grad = pos_weight[:, None] * query
    neg_grad = lax.dot_general(neg_weight, query_half, (((0,), (0,)), ((), ())), preferred_element_type=jnp.float32)
    per_row = jnp.concatenate([head_grad, tail_grad, neg_grad], axis=0)
    per_row = jnp.where(valid[:, None], per_row, jnp.zeros((), jnp.float32))
    return jax.ops.segment_sum(per_row, flat, num_segments=rows.shape[0])


def reference(table, relations, req_rows, owner_count, owner_start, head_slot, rel_id, tail_slot, neg_slot):
    owners = OWNERS
    cap = CAP
    heads = head_slot.reshape(owners, B_DEV)
    tails = tail_slot.reshape(owners, B_DEV)
    negs = neg_slot.reshape(owners, NEG)
    rels = rel_id.reshape(owners, B_DEV)
    column = jnp.arange(cap, dtype=jnp.int32)
    owner_ids = jnp.arange(owners, dtype=jnp.int32)

    def device(grad, p):
        count = owner_count[p]
        start = owner_start[p]
        packed = req_rows[p]
        live = column[None, :] < count[:, None]
        where_at = jnp.clip(start[:, None] + column[None, :], 0, SLOTS - 1).astype(jnp.int32)
        local = jnp.where(live, jnp.take(packed, where_at), 0).astype(jnp.int32)
        global_ids = (owner_ids[:, None] * ENT_DEV + local).reshape(-1).astype(jnp.int32)
        rows = jnp.where(live.reshape(-1, 1), jnp.take(table, global_ids, axis=0), jnp.zeros((), jnp.bfloat16))
        lookups = jnp.concatenate([heads[p], tails[p], negs[p]]).astype(jnp.int32)
        flat, valid = locate(lookups, start, count, cap)
        rel_rows = jnp.take(relations, rels[p], axis=0)
        grads = slot_gradients(rows, flat, valid, rel_rows, B_DEV)
        return grad.at[global_ids].add(grads), None

    total = jnp.zeros((ENTITIES, D), jnp.float32)
    total, _ = lax.scan(device, total, jnp.arange(owners, dtype=jnp.int32))
    return total
```

```python
import jax
import jax.numpy as jnp
from jax import lax
from jax.experimental import pallas as pl
from jax.experimental.pallas import tpu as pltpu
from jax.sharding import PartitionSpec as P

MESH = pl.DeviceIdType.MESH
CAP = 16
GROUP = 16
GROUPS = 8
SPAN = CAP * GROUP
LANES = 128
F32 = jnp.float32
BF16 = jnp.bfloat16


def onehot(match):
    return jnp.where(match, 1.0, 0.0).astype(BF16)


def column(row):
    return jnp.transpose(jnp.broadcast_to(row, (LANES, LANES)))


def iota(shape, axis):
    return lax.broadcasted_iota(jnp.int32, shape, axis)


def kernel(
    table_h, rel_h, req_h, count_h, start_h, head_h, relid_h, tail_h, neg_h,
    out_ref,
    table, rel, req, count, start, look, relid,
    slotrow, slotcol, reqrow, lookcol, relcol, lookrow,
    idxbuf, wantrow, found, rows, rvec, emb, negb, qhalf, nweight, perrow, sent, back,
    local_sem, id_send, id_recv, row_send, row_recv, grad_send, grad_recv,
):
    w = lax.axis_index("wide")
    y = lax.axis_index("narrow")
    x, z, core = w // 8, (w // 2) % 4, w % 2
    ahead = ([(x + d) % 4 * 8 for d in range(4)], [(z + d) % 4 * 2 for d in range(4)])
    behind = ([(x + 4 - d) % 4 * 8 for d in range(4)], [(z + 4 - d) % 4 * 2 for d in range(4)])

    def each_partner(g, forward, act):
        t, c = g // 2, g % 2
        cc = (core + c) % 2
        xs, zs = ahead if forward else behind
        if forward:
            ys = [(y + t + 8 - m) % 4 for m in range(4)]
        else:
            ys = [(y + 8 - t + m) % 4 for m in range(4)]
        for u in range(GROUP):
            dx, dz = u // 4, u % 4
            device = (xs[dx] + zs[dz] + cc, ys[(dx + dz) % 4])
            if u == 0:
                pl.when(g > 0)(lambda device=device: act(0, device))
            else:
                act(u, device)

    barrier = pltpu.get_barrier_semaphore()

    @pl.loop(0, GROUPS)
    def _(g):
        each_partner(
            g, True, lambda u, device: pl.semaphore_signal(barrier, inc=1, device_id=device, device_id_type=MESH)
        )

    loads = [
        (start_h, start), (count_h, count), (req_h, req),
        (head_h, look.at[pl.ds(0, 8)]), (tail_h, look.at[pl.ds(8, 8)]), (neg_h, look.at[pl.ds(16, 8)]),
        (relid_h, relid), (table_h, table), (rel_h, rel),
    ]
    copies = [pltpu.make_async_copy(a, b, local_sem.at[i]) for i, (a, b) in enumerate(loads)]
    for copy in copies:
        copy.start()
    for copy in copies[:7]:
        copy.wait()

    row16 = iota((16, LANES), 0)
    first, many = start[...], count[...]
    facts = jnp.where(row16 == 0, first >> 6, jnp.where(row16 == 1, first & 63, jnp.where(row16 == 2, many, 0)))
    facts = facts.astype(F32).astype(BF16)
    asked = req[...]
    digits = jnp.concatenate([asked >> 5, asked & 31], axis=0).astype(F32).astype(BF16)
    down = iota((LANES, LANES), 0)

    @pl.loop(0, 16)
    def _(r):
        lane = iota((1, LANES), 1)
        k = r * 8 + (lane >> 4)
        c = lane & 15
        t, cc, u = k >> 5, (k >> 4) & 1, k & 15
        dx, dz = u >> 2, u & 3
        dy = (t - dx - dz) & 3
        owner = ((((x + dx) & 3) * 4 + ((z + dz) & 3)) * 2 + ((core + cc) & 1)) * 4 + ((y + dy) & 3)
        known = jnp.dot(facts, onehot(down == owner), preferred_element_type=F32)
        slot = (known[0:1] * 64.0 + known[1:2]).astype(jnp.int32) + c
        live = c < known[2:3].astype(jnp.int32)
        place = jnp.where(live, slot, -1).astype(F32)
        slotrow[pl.ds(r, 1)] = place
        slotcol[pl.ds(pl.multiple_of(r * LANES, LANES), LANES)] = column(place)
        picked = jnp.dot(digits, onehot(down == (slot & 127)), preferred_element_type=F32)
        mine = row16 == (slot >> 7)
        high = jnp.sum(jnp.where(mine, picked[:16], 0.0), axis=0, keepdims=True)
        low = jnp.sum(jnp.where(mine, picked[16:], 0.0), axis=0, keepdims=True)
        reqrow[pl.ds(r, 1)] = jnp.where(live, high * 32.0 + low, 0.0)

    lookrow[...] = look[...].astype(F32)

    pl.semaphore_wait(barrier, GROUPS * GROUP - 1)

    @pl.loop(0, GROUPS)
    def _(g):
        def send(u, device):
            pltpu.make_async_remote_copy(
                src_ref=reqrow.at[pl.ds(g * 2 + u // 8, 1)],
                dst_ref=idxbuf.at[pl.ds(g * GROUP + u, 1)],
                send_sem=id_send,
                recv_sem=id_recv.at[g],
                device_id=device,
                device_id_type=MESH,
            ).start()

        each_partner(g, True, send)

    idxbuf[0:1] = reqrow[0:1]

    @pl.loop(0, 24)
    def _(i):
        lookcol[pl.ds(pl.multiple_of(i * LANES, LANES), LANES)] = column(lookrow[pl.ds(i, 1)])

    @pl.loop(0, 8)
    def _(i):
        relcol[pl.ds(pl.multiple_of(i * LANES, LANES), LANES)] = column(relid[pl.ds(i, 1)].astype(F32))

    copies[7].wait()
    some_device = (ahead[0][1] + ahead[1][0] + core, y)

    def arrived(buf, sem, g, unit):
        def wait(first, n):
            part = buf.at[pl.ds(pl.multiple_of(first * unit, unit), n * unit)]
            pltpu.make_async_remote_copy(
                src_ref=part, dst_ref=part, send_sem=sem.at[g], recv_sem=sem.at[g],
                device_id=some_device, device_id_type=MESH,
            ).wait_recv()

        pl.when(g == 0)(lambda: wait(1, GROUP - 1))
        pl.when(g > 0)(lambda: wait(g * GROUP, GROUP))

    def drained(buf, sem, unit):
        n = GROUPS * GROUP - 1
        part = buf.at[pl.ds(unit, n * unit)]
        pltpu.make_async_remote_copy(
            src_ref=part, dst_ref=part, send_sem=sem, recv_sem=sem, device_id=some_device, device_id_type=MESH
        ).wait_send()

    def send_blocks(src, dst, send_sem, recv_sem, g, forward):
        def send(u, device):
            at = pl.ds(pl.multiple_of((g * GROUP + u) * CAP, CAP), CAP)
            pltpu.make_async_remote_copy(
                src_ref=src.at[at], dst_ref=dst.at[at], send_sem=send_sem, recv_sem=recv_sem.at[g],
                device_id=device, device_id_type=MESH,
            ).start()

        each_partner(g, forward, send)

    @pl.loop(0, GROUPS)
    def _(g):
        arrived(idxbuf, id_recv, g, 1)
        belongs = (iota((8, LANES), 1) >> 4) == iota((8, LANES), 0)
        halves = []
        for h in range(2):
            got = idxbuf[pl.ds(pl.multiple_of(g * 16 + h * 8, 8), 8)]
            row = jnp.sum(jnp.where(belongs, got, 0.0), axis=0, keepdims=True)
            wantrow[pl.ds(g * 2 + h, 1)] = row
            halves.append(column(row).astype(jnp.int32))
        want = jnp.concatenate(halves, axis=0)
        across = iota((SPAN, LANES), 1)
        pick = jnp.concatenate([onehot(want == across + i * LANES) for i in range(8)], axis=1)
        here = jnp.dot(pick, table[...], preferred_element_type=F32).astype(BF16)
        found[pl.ds(pl.multiple_of(g * SPAN, SPAN), SPAN)] = here
        send_blocks(found, rows, row_send, row_recv, g, False)

    rows[0:CAP] = found[0:CAP]

    copies[8].wait()
    rvec[...] = jnp.zeros_like(rvec)

    @pl.loop(0, rel.shape[0] // 256)
    def _(q):
        across = (iota((1024, LANES), 1) + q * 256).astype(F32)
        ids = relcol[...]
        pick = jnp.concatenate([onehot(ids == across), onehot(ids == across + 128.0)], axis=1)
        rvec[...] += jnp.dot(pick, rel[pl.ds(pl.multiple_of(q * 256, 256), 256)], preferred_element_type=F32)

    emb[...] = jnp.zeros_like(emb)

    @pl.loop(0, GROUPS)
    def _(g):
        arrived(rows, row_recv, g, CAP)

        @pl.loop(0, 3)
        def _(b):
            at = pl.ds(pl.multiple_of(b * 1024, 1024), 1024)
            ids = lookcol[at]
            pick = jnp.concatenate([onehot(ids == slotrow[pl.ds(g * 2 + h, 1)]) for h in range(2)], axis=1)
            emb[at] += jnp.dot(pick, rows[pl.ds(pl.multiple_of(g * SPAN, SPAN), SPAN)], preferred_element_type=F32)

    negb[...] = emb[2048:].astype(BF16)

    @pl.loop(0, 4)
    def _(b):
        at = pl.ds(pl.multiple_of(b * 256, 256), 256)
        r = rvec[at]
        query = emb[at] * r
        half = query.astype(BF16)
        qhalf[at] = half
        tail = emb[pl.ds(pl.multiple_of(1024 + b * 256, 256), 256)]
        positive = jnp.sum(query * tail, axis=1, keepdims=True)
        pos_weight = -1.0 / (1.0 + jnp.exp(positive))
        perrow[pl.ds(pl.multiple_of(1024 + b * 256, 256), 256)] = (pos_weight * query).astype(BF16)
        score = lax.dot_general(half, negb[...], (((1,), (1,)), ((), ())), preferred_element_type=F32)
        weight = (1.0 / (1.0 + jnp.exp(-score))).astype(BF16)
        nweight[at] = weight
        pulled = jnp.dot(weight, negb[...], preferred_element_type=F32)
        perrow[at] = (r * (pos_weight * tail + pulled)).astype(BF16)

    perrow[2048:] = lax.dot_general(
        nweight[...], qhalf[...], (((0,), (0,)), ((), ())), preferred_element_type=F32
    ).astype(BF16)

    @pl.loop(0, GROUPS)
    def _(g):
        at = pl.ds(pl.multiple_of(g * SPAN, SPAN), SPAN)
        place = slotcol[at]
        pick = jnp.concatenate([onehot(place == lookrow[i : i + 1]) for i in range(24)], axis=1)
        sent[at] = jnp.dot(pick, perrow[...], preferred_element_type=F32).astype(BF16)
        send_blocks(sent, back, grad_send, grad_recv, g, True)

    back[0:CAP] = sent[0:CAP]
    out_ref[...] = jnp.zeros_like(out_ref)

    @pl.loop(0, GROUPS)
    def _(g):
        arrived(back, grad_recv, g, CAP)
        down = iota((1024, LANES), 0).astype(F32)
        pick = jnp.concatenate([onehot(down == wantrow[pl.ds(g * 2 + h, 1)]) for h in range(2)], axis=1)
        out_ref[...] += jnp.dot(
            pick, back[pl.ds(pl.multiple_of(g * SPAN, SPAN), SPAN)], preferred_element_type=F32
        )

    drained(idxbuf, id_send, 1)
    drained(found, row_send, CAP)
    drained(sent, grad_send, CAP)


def per_device(table, relations, req_rows, owner_count, owner_start, head_slot, rel_id, tail_slot, neg_slot):
    ents, width = table.shape
    slots = req_rows.shape[1]
    batch = head_slot.shape[0]
    vmem = pltpu.VMEM
    dma = pltpu.SemaphoreType.DMA
    scratch = [
        vmem((ents, width), BF16), vmem(relations.shape, BF16), vmem((16, LANES), jnp.int32),
        vmem((1, LANES), jnp.int32), vmem((1, LANES), jnp.int32), vmem((24, LANES), jnp.int32),
        vmem((8, LANES), jnp.int32),
        vmem((16, LANES), F32), vmem((slots, LANES), F32), vmem((16, LANES), F32),
        vmem((3 * batch, LANES), F32), vmem((batch, LANES), F32), vmem((24, LANES), F32),
        vmem((128, LANES), F32), vmem((16, LANES), F32), vmem((slots, width), BF16), vmem((slots, width), BF16),
        vmem((batch, width), F32), vmem((3 * batch, width), F32), vmem((batch, width), BF16),
        vmem((batch, width), BF16), vmem((batch, batch), BF16), vmem((3 * batch, width), BF16),
        vmem((slots, width), BF16), vmem((slots, width), BF16),
        dma((9,)), dma, dma((GROUPS,)), dma, dma((GROUPS,)), dma, dma((GROUPS,)),
    ]
    return pl.pallas_call(
        kernel,
        out_shape=jax.ShapeDtypeStruct((ents, width), F32),
        in_specs=[pl.BlockSpec(memory_space=pl.ANY)] * 9,
        out_specs=pl.BlockSpec(memory_space=pltpu.VMEM),
        scratch_shapes=scratch,
        compiler_params=pltpu.CompilerParams(
            collective_id=0, has_side_effects=True, vmem_limit_bytes=60 * 2**20
        ),
        name="distmult_step",
    )(
        table,
        relations,
        req_rows.reshape(16, LANES),
        owner_count,
        owner_start,
        head_slot.reshape(8, LANES),
        rel_id.reshape(8, LANES),
        tail_slot.reshape(8, LANES),
        neg_slot.reshape(8, LANES),
    )


def solution(mesh):
    both = ("wide", "narrow")
    in_specs = (P(both, None), P(), P(both, None), P(both, None), P(both, None), P(both), P(both), P(both), P(both))
    return jax.shard_map(per_device, mesh=mesh, in_specs=in_specs, out_specs=P(both, None), check_vma=False)
```

```python
import jax
import jax.numpy as jnp
from jax import lax
from jax.experimental import pallas as pl
from jax.experimental.pallas import tpu as pltpu
from jax.sharding import PartitionSpec as P

MESH = pl.DeviceIdType.MESH
CAP = 16
SLOTS = 2048
RELATION_PARTS = 8
GROUP = 16
GROUPS = 8
SPAN = CAP * GROUP
LANES = 128
F32 = jnp.float32
ROW_ORDER = (0, 1, 7, 6, 5, 4, 3, 2)


def partner_offsets():
    every = [(dx, dz, dy, dc) for dx in range(4) for dz in range(4) for dy in range(4) for dc in range(2)]
    hops = [sum(min(d, 4 - d) for d in o[:3]) for o in every]
    return [every[i] for i in sorted(range(len(every)), key=lambda i: (hops[i], i * 37 % 128))]


OFFSETS = partner_offsets()


def packed(digits):
    word = sum(d << (4 * i) for i, d in enumerate(digits))
    return word - (1 << 32) if word >= 1 << 31 else word


BF16 = jnp.bfloat16


def onehot(match):
    return jnp.where(match, 1.0, 0.0).astype(BF16)


def column(row):
    return jnp.transpose(jnp.broadcast_to(row, (LANES, LANES)))


def iota(shape, axis):
    return lax.broadcasted_iota(jnp.int32, shape, axis)


def kernel(
    table_h, rel_h, req_h, count_h, start_h, head_h, relid_h, tail_h, neg_h, offsets_h,
    out_ref,
    table, rel, req, count, start, look, relid, offsets,
    slotrow, slotcol, reqrow, lookcol, relwide, lookrow,
    idxbuf, wantrow, found, rows, rvec, emb, negb, qhalf, nweight, perrow, sent, back,
    local_sem, rel_sem, id_send, id_recv, row_send, row_recv, grad_send, grad_recv,
):
    w = lax.axis_index("wide")
    y = lax.axis_index("narrow")
    x, z, core = w // 8, (w // 2) % 4, w % 2

    xs, zs = [((x + d) & 3) * 8 for d in range(4)], [((z + d) & 3) * 2 + core for d in range(4)]
    ys, cores = [(y + d) & 3 for d in range(4)], [0, 1 - 2 * core]

    def partner(n):
        dx, dz, dy, dc = OFFSETS[n]
        return (xs[dx] + zs[dz] + cores[dc], ys[dy])

    def each_partner(g, sign, act):
        for u in range(GROUP):
            members = [OFFSETS[i * GROUP + u] for i in range(GROUPS)]
            xz = (packed([o[0] * 4 + o[1] for o in members]) >> (g * 4)) & 15
            yc = (packed([o[2] * 2 + o[3] for o in members]) >> (g * 4)) & 15
            px = (x + sign * (xz >> 2)) & 3
            pz = (z + sign * (xz & 3)) & 3
            py = (y + sign * (yc >> 1)) & 3
            device = (px * 8 + pz * 2 + ((core + yc) & 1), py)
            if u == 0:
                pl.when(g > 0)(lambda device=device: act(0, device))
            else:
                act(u, device)

    loads = [
        (start_h, start), (count_h, count), (req_h, req), (offsets_h, offsets), (table_h, table),
        (head_h, look.at[pl.ds(0, 8)]), (tail_h, look.at[pl.ds(8, 8)]), (neg_h, look.at[pl.ds(16, 8)]),
        (relid_h, relid),
    ]
    copies = [pltpu.make_async_copy(a, b, local_sem.at[i]) for i, (a, b) in enumerate(loads)]
    part = rel.shape[1]

    def load_relations(q):
        return pltpu.make_async_copy(
            rel_h.at[pl.ds(pl.multiple_of(q * part, part), part)], rel.at[q % 4], rel_sem.at[q % 4]
        )

    for copy in copies:
        copy.start()
    for q in range(4):
        load_relations(q).start()
    barrier = pltpu.get_barrier_semaphore()
    for n in range(GROUPS * GROUP - 1, 0, -1):
        pl.semaphore_signal(barrier, inc=1, device_id=partner(n), device_id_type=MESH)

    for copy in copies[:5]:
        copy.wait()

    row16 = iota((16, LANES), 0)
    first, many = start[...], count[...]
    facts = jnp.where(row16 == 0, first >> 6, jnp.where(row16 == 1, first & 63, jnp.where(row16 == 2, many, 0)))
    facts = facts.astype(F32).astype(BF16)
    asked = req[...]
    digits = jnp.concatenate([asked >> 5, asked & 31], axis=0).astype(F32).astype(BF16)
    lane = iota((1, SLOTS), 1)
    down = iota((LANES, SLOTS), 0)
    c = lane & 15
    off = offsets[...]
    ox, oz, oy, oc = off & 3, (off >> 2) & 3, (off >> 4) & 3, off >> 6
    owner = ((((x + ox) & 3) * 4 + ((z + oz) & 3)) * 2 + ((core + oc) & 1)) * 4 + ((y + oy) & 3)
    known = jnp.dot(facts, onehot(down == owner), preferred_element_type=F32)
    slot = (known[0:1] * 64.0 + known[1:2]).astype(jnp.int32) + c
    live = c < known[2:3].astype(jnp.int32)
    place = jnp.where(live, slot, -1).astype(F32)
    picked = jnp.dot(digits, onehot(down == (slot & 127)), preferred_element_type=F32)
    mine = iota((16, SLOTS), 0) == (slot >> 7)
    high = jnp.sum(jnp.where(mine, picked[:16], 0.0), axis=0, keepdims=True)
    low = jnp.sum(jnp.where(mine, picked[16:], 0.0), axis=0, keepdims=True)
    wanted = jnp.where(live, high * 32.0 + low, 0.0)
    for r in range(16):
        slotrow[r : r + 1] = place[:, r * LANES : (r + 1) * LANES]
        reqrow[r : r + 1] = wanted[:, r * LANES : (r + 1) * LANES]

    pl.semaphore_wait(barrier, GROUPS * GROUP - 1)

    for n in [g * GROUP + u for g in ROW_ORDER for u in range(GROUP)][1:]:
        pltpu.make_async_remote_copy(
            src_ref=reqrow.at[pl.ds(n // 8, 1)],
            dst_ref=idxbuf.at[pl.ds(n, 1)],
            send_sem=id_send,
            recv_sem=id_recv.at[n // GROUP],
            device_id=partner(n),
            device_id_type=MESH,
        ).start()

    idxbuf[0:1] = reqrow[0:1]

    some_device = partner(2)

    def arrived(buf, sem, g, unit):
        def wait(first, n):
            part = buf.at[pl.ds(pl.multiple_of(first * unit, unit), n * unit)]
            pltpu.make_async_remote_copy(
                src_ref=part, dst_ref=part, send_sem=sem.at[g], recv_sem=sem.at[g],
                device_id=some_device, device_id_type=MESH,
            ).wait_recv()

        pl.when(g == 0)(lambda: wait(1, GROUP - 1))
        pl.when(g > 0)(lambda: wait(g * GROUP, GROUP))

    def drained(buf, sem, unit):
        n = GROUPS * GROUP - 1
        part = buf.at[pl.ds(unit, n * unit)]
        pltpu.make_async_remote_copy(
            src_ref=part, dst_ref=part, send_sem=sem, recv_sem=sem, device_id=some_device, device_id_type=MESH
        ).wait_send()

    def send_blocks(src, dst, send_sem, recv_sem, g, sign):
        def send(u, device):
            at = pl.ds(pl.multiple_of((g * GROUP + u) * CAP, CAP), CAP)
            pltpu.make_async_remote_copy(
                src_ref=src.at[at], dst_ref=dst.at[at], send_sem=send_sem, recv_sem=recv_sem.at[g],
                device_id=device, device_id_type=MESH,
            ).start()

        each_partner(g, sign, send)

    for copy in copies[5:9]:
        copy.wait()
    lookrow[...] = look[...].astype(F32)

    def columns(dst, src, n):
        @pl.loop(0, n // 8)
        def _(i):
            for e in range(8):
                at = pl.ds(pl.multiple_of((i * 8 + e) * LANES, LANES), LANES)
                dst[at] = column(src[pl.ds(i * 8 + e, 1)])

    columns(lookcol, lookrow, 24)
    columns(slotcol, slotrow, 16)

    @pl.loop(0, GROUPS)
    def _(i):
        g = (packed(ROW_ORDER) >> (i * 4)) & 15
        arrived(idxbuf, id_recv, g, 1)
        belongs = (iota((8, LANES), 1) >> 4) == iota((8, LANES), 0)
        halves = []
        for h in range(2):
            got = idxbuf[pl.ds(pl.multiple_of(g * 16 + h * 8, 8), 8)]
            row = jnp.sum(jnp.where(belongs, got, 0.0), axis=0, keepdims=True)
            wantrow[pl.ds(g * 2 + h, 1)] = row
            halves.append(column(row).astype(jnp.int32))
        want = jnp.concatenate(halves, axis=0)
        across = iota((SPAN, LANES), 1)
        pick = jnp.concatenate([onehot(want == across + n * LANES) for n in range(8)], axis=1)
        here = jnp.dot(pick, table[...], preferred_element_type=F32).astype(BF16)
        found[pl.ds(pl.multiple_of(g * SPAN, SPAN), SPAN)] = here
        send_blocks(found, rows, row_send, row_recv, g, -1)

    rows[0:CAP] = found[0:CAP]

    @pl.loop(0, RELATION_PARTS)
    def _(q):
        load_relations(q).wait()
        for e in range(4):
            rows_at = pl.ds(pl.multiple_of(q * part + e * (part // 4), 8), part // 4)
            relwide[rows_at] = rel[q % 4, pl.ds(e * (part // 4), part // 4)].astype(F32)
        pl.when(q + 4 < RELATION_PARTS)(lambda: load_relations(q + 4).start())

    @pl.loop(0, rvec.shape[0] // 8)
    def _(i):
        for e in range(8):
            row = relid[i // 16, (i % 16) * 8 + e]
            rvec[pl.ds(i * 8 + e, 1)] = relwide[pl.ds(row, 1)]

    emb[...] = jnp.zeros_like(emb)

    @pl.loop(0, GROUPS)
    def _(i):
        g = (packed(ROW_ORDER) >> (i * 4)) & 15
        arrived(rows, row_recv, g, CAP)

        @pl.loop(0, 3)
        def _(b):
            at = pl.ds(pl.multiple_of(b * 1024, 1024), 1024)
            ids = lookcol[at]
            pick = jnp.concatenate([onehot(ids == slotrow[pl.ds(g * 2 + h, 1)]) for h in range(2)], axis=1)
            emb[at] += jnp.dot(pick, rows[pl.ds(pl.multiple_of(g * SPAN, SPAN), SPAN)], preferred_element_type=F32)

    negb[...] = emb[2048:].astype(BF16)

    @pl.loop(0, 4)
    def _(b):
        at = pl.ds(pl.multiple_of(b * 256, 256), 256)
        r = rvec[at]
        query = emb[at] * r
        half = query.astype(BF16)
        qhalf[at] = half
        tail = emb[pl.ds(pl.multiple_of(1024 + b * 256, 256), 256)]
        positive = jnp.sum(query * tail, axis=1, keepdims=True)
        pos_weight = -1.0 / (1.0 + jnp.exp(positive))
        perrow[pl.ds(pl.multiple_of(1024 + b * 256, 256), 256)] = (pos_weight * query).astype(BF16)
        score = lax.dot_general(half, negb[...], (((1,), (1,)), ((), ())), preferred_element_type=F32)
        weight = (1.0 / (1.0 + jnp.exp(-score))).astype(BF16)
        nweight[at] = weight
        pulled = jnp.dot(weight, negb[...], preferred_element_type=F32)
        perrow[at] = (r * (pos_weight * tail + pulled)).astype(BF16)

    perrow[2048:] = lax.dot_general(
        nweight[...], qhalf[...], (((0,), (0,)), ((), ())), preferred_element_type=F32
    ).astype(BF16)

    @pl.loop(0, GROUPS)
    def _(i):
        g = GROUPS - 1 - i
        at = pl.ds(pl.multiple_of(g * SPAN, SPAN), SPAN)
        place = slotcol[at]
        pick = jnp.concatenate([onehot(place == lookrow[n : n + 1]) for n in range(24)], axis=1)
        sent[at] = jnp.dot(pick, perrow[...], preferred_element_type=F32).astype(BF16)
        send_blocks(sent, back, grad_send, grad_recv, g, 1)

    back[0:CAP] = sent[0:CAP]
    out_ref[...] = jnp.zeros_like(out_ref)

    @pl.loop(0, GROUPS)
    def _(i):
        g = GROUPS - 1 - i
        arrived(back, grad_recv, g, CAP)
        down = iota((1024, LANES), 0).astype(F32)
        pick = jnp.concatenate([onehot(down == wantrow[pl.ds(g * 2 + h, 1)]) for h in range(2)], axis=1)
        out_ref[...] += jnp.dot(
            pick, back[pl.ds(pl.multiple_of(g * SPAN, SPAN), SPAN)], preferred_element_type=F32
        )

    drained(idxbuf, id_send, 1)
    drained(found, row_send, CAP)
    drained(sent, grad_send, CAP)


def per_device(table, relations, req_rows, owner_count, owner_start, head_slot, rel_id, tail_slot, neg_slot):
    ents, width = table.shape
    slots = req_rows.shape[1]
    batch = head_slot.shape[0]
    vmem = pltpu.VMEM
    dma = pltpu.SemaphoreType.DMA
    scratch = [
        vmem((ents, width), BF16), vmem((4, relations.shape[0] // RELATION_PARTS, width), BF16), vmem((16, LANES), jnp.int32),
        vmem((1, LANES), jnp.int32), vmem((1, LANES), jnp.int32), vmem((24, LANES), jnp.int32),
        pltpu.SMEM((8, LANES), jnp.int32), vmem((1, slots), jnp.int32),
        vmem((16, LANES), F32), vmem((slots, LANES), F32), vmem((16, LANES), F32),
        vmem((3 * batch, LANES), F32), vmem(relations.shape, F32), vmem((24, LANES), F32),
        vmem((128, LANES), F32), vmem((16, LANES), F32), vmem((slots, width), BF16), vmem((slots, width), BF16),
        vmem((batch, width), F32), vmem((3 * batch, width), F32), vmem((batch, width), BF16),
        vmem((batch, width), BF16), vmem((batch, batch), BF16), vmem((3 * batch, width), BF16),
        vmem((slots, width), BF16), vmem((slots, width), BF16),
        dma((9,)), dma((4,)), dma, dma((GROUPS,)), dma, dma((GROUPS,)), dma, dma((GROUPS,)),
    ]
    return pl.pallas_call(
        kernel,
        out_shape=jax.ShapeDtypeStruct((ents, width), F32),
        in_specs=[pl.BlockSpec(memory_space=pltpu.HBM)] * 10,
        out_specs=pl.BlockSpec(memory_space=pltpu.VMEM),
        scratch_shapes=scratch,
        compiler_params=pltpu.CompilerParams(
            collective_id=0, has_side_effects=True, vmem_limit_bytes=50 * 2**20
        ),
        name="distmult_step",
    )(*[pltpu.with_memory_space_constraint(v, pltpu.HBM) for v in (
        table,
        relations,
        req_rows.reshape(16, LANES),
        owner_count,
        owner_start,
        head_slot.reshape(8, LANES),
        rel_id.reshape(8, LANES),
        tail_slot.reshape(8, LANES),
        neg_slot.reshape(8, LANES),
        jnp.asarray([[o[0] | o[1] << 2 | o[2] << 4 | o[3] << 6 for o in OFFSETS for _ in range(CAP)]], jnp.int32),
    )])


def solution(mesh):
    both = ("wide", "narrow")
    in_specs = (P(both, None), P(), P(both, None), P(both, None), P(both, None), P(both), P(both), P(both), P(both))
    return jax.shard_map(per_device, mesh=mesh, in_specs=in_specs, out_specs=P(both, None), check_vma=False)
```

```python
import jax
import jax.numpy as jnp
from jax import lax
from jax.experimental import pallas as pl
from jax.experimental.pallas import tpu as pltpu
from jax.sharding import PartitionSpec as P

MESH = pl.DeviceIdType.MESH
CAP = 16
SLOTS = 2048
RELATION_PARTS = 8
GROUP = 16
GROUPS = 8
SPAN = CAP * GROUP
LANES = 128
F32 = jnp.float32


def hops(offset):
    return sum(min(d, 4 - d) for d in offset[:3])


def partner_offsets():
    offsets = []
    for g in range(GROUPS):
        members = [(i // 4, i % 4, (g // 2 - i // 4 - i % 4) % 4, g % 2) for i in range(GROUP)]
        members.sort(key=lambda o: (o != (0, 0, 0, 0), -hops(o)))
        offsets += members
    return offsets


OFFSETS = partner_offsets()


def packed(digits):
    word = sum(d << (4 * i) for i, d in enumerate(digits))
    return word - (1 << 32) if word >= 1 << 31 else word


BF16 = jnp.bfloat16


def onehot(match):
    return jnp.where(match, 1.0, 0.0).astype(BF16)


def column(row):
    return jnp.transpose(jnp.broadcast_to(row, (LANES, LANES)))


def iota(shape, axis):
    return lax.broadcasted_iota(jnp.int32, shape, axis)


def kernel(
    table_h, rel_h, req_h, count_h, start_h, head_h, relid_h, tail_h, neg_h, offsets_h,
    out_ref,
    table, rel, req, count, start, look, relid, offsets,
    slotrow, slotcol, reqrow, lookcol, relwide, lookrow,
    idxbuf, wantrow, found, rows, rvec, emb, negb, qhalf, nweight, perrow, sent, back,
    local_sem, rel_sem, id_send, id_recv, row_send, row_recv, grad_send, grad_recv,
):
    w = lax.axis_index("wide")
    y = lax.axis_index("narrow")
    x, z, core = w // 8, (w // 2) % 4, w % 2

    xs, zs = [((x + d) & 3) * 8 for d in range(4)], [((z + d) & 3) * 2 + core for d in range(4)]
    ys, cores = [(y + d) & 3 for d in range(4)], [0, 1 - 2 * core]

    def partner(n):
        dx, dz, dy, dc = OFFSETS[n]
        return (xs[dx] + zs[dz] + cores[dc], ys[dy])

    def each_partner(g, half, sign, act):
        for u in range(half * 8, half * 8 + 8):
            members = [OFFSETS[i * GROUP + u] for i in range(GROUPS)]
            xz = (packed([o[0] * 4 + o[1] for o in members]) >> (g * 4)) & 15
            yc = (packed([o[2] * 2 + o[3] for o in members]) >> (g * 4)) & 15
            px = (x + sign * (xz >> 2)) & 3
            pz = (z + sign * (xz & 3)) & 3
            py = (y + sign * (yc >> 1)) & 3
            device = (px * 8 + pz * 2 + ((core + yc) & 1), py)
            if u == 0:
                pl.when(g > 0)(lambda device=device: act(0, device))
            else:
                act(u, device)

    loads = [
        (start_h, start), (count_h, count), (req_h, req), (offsets_h, offsets), (table_h, table),
        (head_h, look.at[pl.ds(0, 8)]), (tail_h, look.at[pl.ds(8, 8)]), (neg_h, look.at[pl.ds(16, 8)]),
        (relid_h, relid),
    ]
    copies = [pltpu.make_async_copy(a, b, local_sem.at[i]) for i, (a, b) in enumerate(loads)]
    part = rel.shape[1]

    def load_relations(q):
        return pltpu.make_async_copy(
            rel_h.at[pl.ds(pl.multiple_of(q * part, part), part)], rel.at[q % 4], rel_sem.at[q % 4]
        )

    for copy in copies:
        copy.start()
    for q in range(4):
        load_relations(q).start()
    barrier = pltpu.get_barrier_semaphore()
    for n in sorted(range(1, GROUPS * GROUP), key=lambda n: -hops(OFFSETS[n])):
        pl.semaphore_signal(barrier, inc=1, device_id=partner(n), device_id_type=MESH)

    for copy in copies[:5]:
        copy.wait()

    row16 = iota((16, LANES), 0)
    first, many = start[...], count[...]
    facts = jnp.where(row16 == 0, first >> 6, jnp.where(row16 == 1, first & 63, jnp.where(row16 == 2, many, 0)))
    facts = facts.astype(F32).astype(BF16)
    asked = req[...]
    digits = jnp.concatenate([asked >> 5, asked & 31], axis=0).astype(F32).astype(BF16)
    lane = iota((1, SLOTS), 1)
    down = iota((LANES, SLOTS), 0)
    c = lane & 15
    off = offsets[...]
    ox, oz, oy, oc = off & 3, (off >> 2) & 3, (off >> 4) & 3, off >> 6
    owner = ((((x + ox) & 3) * 4 + ((z + oz) & 3)) * 2 + ((core + oc) & 1)) * 4 + ((y + oy) & 3)
    known = jnp.dot(facts, onehot(down == owner), preferred_element_type=F32)
    slot = (known[0:1] * 64.0 + known[1:2]).astype(jnp.int32) + c
    live = c < known[2:3].astype(jnp.int32)
    place = jnp.where(live, slot, -1).astype(F32)
    picked = jnp.dot(digits, onehot(down == (slot & 127)), preferred_element_type=F32)
    mine = iota((16, SLOTS), 0) == (slot >> 7)
    high = jnp.sum(jnp.where(mine, picked[:16], 0.0), axis=0, keepdims=True)
    low = jnp.sum(jnp.where(mine, picked[16:], 0.0), axis=0, keepdims=True)
    wanted = jnp.where(live, high * 32.0 + low, 0.0)
    for r in range(16):
        slotrow[r : r + 1] = place[:, r * LANES : (r + 1) * LANES]
        reqrow[r : r + 1] = wanted[:, r * LANES : (r + 1) * LANES]

    pl.semaphore_wait(barrier, GROUPS * GROUP - 1)

    for n in range(1, GROUPS * GROUP):
        pltpu.make_async_remote_copy(
            src_ref=reqrow.at[pl.ds(n // 8, 1)],
            dst_ref=idxbuf.at[pl.ds(n, 1)],
            send_sem=id_send,
            recv_sem=id_recv.at[n // GROUP],
            device_id=partner(n),
            device_id_type=MESH,
        ).start()

    idxbuf[0:1] = reqrow[0:1]

    some_device = partner(2)

    def arrived(buf, sem, g, unit):
        def wait(first, n):
            part = buf.at[pl.ds(pl.multiple_of(first * unit, unit), n * unit)]
            pltpu.make_async_remote_copy(
                src_ref=part, dst_ref=part, send_sem=sem.at[g], recv_sem=sem.at[g],
                device_id=some_device, device_id_type=MESH,
            ).wait_recv()

        pl.when(g == 0)(lambda: wait(1, GROUP - 1))
        pl.when(g > 0)(lambda: wait(g * GROUP, GROUP))

    def drained(buf, sem, unit):
        n = GROUPS * GROUP - 1
        part = buf.at[pl.ds(unit, n * unit)]
        pltpu.make_async_remote_copy(
            src_ref=part, dst_ref=part, send_sem=sem, recv_sem=sem, device_id=some_device, device_id_type=MESH
        ).wait_send()

    def send_blocks(src, dst, send_sem, recv_sem, g, half, sign):
        def send(u, device):
            at = pl.ds(pl.multiple_of((g * GROUP + u) * CAP, CAP), CAP)
            pltpu.make_async_remote_copy(
                src_ref=src.at[at], dst_ref=dst.at[at], send_sem=send_sem, recv_sem=recv_sem.at[g],
                device_id=device, device_id_type=MESH,
            ).start()

        each_partner(g, half, sign, send)

    for copy in copies[5:9]:
        copy.wait()
    lookrow[...] = look[...].astype(F32)

    def columns(dst, src, n):
        @pl.loop(0, n // 8)
        def _(i):
            for e in range(8):
                at = pl.ds(pl.multiple_of((i * 8 + e) * LANES, LANES), LANES)
                dst[at] = column(src[pl.ds(i * 8 + e, 1)])

    columns(lookcol, lookrow, 24)
    columns(slotcol, slotrow, 16)

    @pl.loop(0, GROUPS)
    def _(g):
        arrived(idxbuf, id_recv, g, 1)
        belongs = (iota((8, LANES), 1) >> 4) == iota((8, LANES), 0)
        across = iota((LANES, LANES), 1)
        for half in range(2):
            got = idxbuf[pl.ds(pl.multiple_of(g * 16 + half * 8, 8), 8)]
            row = jnp.sum(jnp.where(belongs, got, 0.0), axis=0, keepdims=True)
            wantrow[pl.ds(g * 2 + half, 1)] = row
            want = column(row).astype(jnp.int32)
            pick = jnp.concatenate([onehot(want == across + n * LANES) for n in range(8)], axis=1)
            here = jnp.dot(pick, table[...], preferred_element_type=F32).astype(BF16)
            found[pl.ds(pl.multiple_of(g * SPAN + half * LANES, LANES), LANES)] = here
            send_blocks(found, rows, row_send, row_recv, g, half, -1)

    rows[0:CAP] = found[0:CAP]

    @pl.loop(0, RELATION_PARTS)
    def _(q):
        load_relations(q).wait()
        for e in range(4):
            rows_at = pl.ds(pl.multiple_of(q * part + e * (part // 4), 8), part // 4)
            relwide[rows_at] = rel[q % 4, pl.ds(e * (part // 4), part // 4)].astype(F32)
        pl.when(q + 4 < RELATION_PARTS)(lambda: load_relations(q + 4).start())

    @pl.loop(0, rvec.shape[0] // 8)
    def _(i):
        for e in range(8):
            row = relid[i // 16, (i % 16) * 8 + e]
            rvec[pl.ds(i * 8 + e, 1)] = relwide[pl.ds(row, 1)]

    emb[...] = jnp.zeros_like(emb)

    @pl.loop(0, GROUPS)
    def _(g):
        arrived(rows, row_recv, g, CAP)

        @pl.loop(0, 3)
        def _(b):
            at = pl.ds(pl.multiple_of(b * 1024, 1024), 1024)
            ids = lookcol[at]
            pick = jnp.concatenate([onehot(ids == slotrow[pl.ds(g * 2 + h, 1)]) for h in range(2)], axis=1)
            emb[at] += jnp.dot(pick, rows[pl.ds(pl.multiple_of(g * SPAN, SPAN), SPAN)], preferred_element_type=F32)

    negb[...] = emb[2048:].astype(BF16)

    for b in range(4):
        at, tail_at = pl.ds(b * 256, 256), pl.ds(1024 + b * 256, 256)
        r = rvec[at]
        query = emb[at] * r
        half = query.astype(BF16)
        qhalf[at] = half
        tail = emb[tail_at]
        positive = jnp.sum(query * tail, axis=1, keepdims=True)
        pos_weight = -1.0 / (1.0 + jnp.exp(positive))
        perrow[tail_at] = (pos_weight * query).astype(BF16)
        score = lax.dot_general(half, negb[...], (((1,), (1,)), ((), ())), preferred_element_type=F32)
        weight = (1.0 / (1.0 + jnp.exp(-score))).astype(BF16)
        nweight[at] = weight
        pulled = jnp.dot(weight, negb[...], preferred_element_type=F32)
        perrow[at] = (r * (pos_weight * tail + pulled)).astype(BF16)

    perrow[2048:] = lax.dot_general(
        nweight[...], qhalf[...], (((0,), (0,)), ((), ())), preferred_element_type=F32
    ).astype(BF16)

    @pl.loop(0, GROUPS)
    def _(i):
        g = GROUPS - 1 - i
        for half in range(2):
            at = pl.ds(pl.multiple_of(g * SPAN + half * LANES, LANES), LANES)
            place = slotcol[at]
            pick = jnp.concatenate([onehot(place == lookrow[n : n + 1]) for n in range(24)], axis=1)
            sent[at] = jnp.dot(pick, perrow[...], preferred_element_type=F32).astype(BF16)
            send_blocks(sent, back, grad_send, grad_recv, g, half, 1)

    back[0:CAP] = sent[0:CAP]
    out_ref[...] = jnp.zeros_like(out_ref)

    @pl.loop(0, GROUPS)
    def _(i):
        g = GROUPS - 1 - i
        arrived(back, grad_recv, g, CAP)
        down = iota((1024, LANES), 0).astype(F32)
        pick = jnp.concatenate([onehot(down == wantrow[pl.ds(g * 2 + h, 1)]) for h in range(2)], axis=1)
        out_ref[...] += jnp.dot(
            pick, back[pl.ds(pl.multiple_of(g * SPAN, SPAN), SPAN)], preferred_element_type=F32
        )

    drained(idxbuf, id_send, 1)
    drained(found, row_send, CAP)
    drained(sent, grad_send, CAP)


def per_device(table, relations, req_rows, owner_count, owner_start, head_slot, rel_id, tail_slot, neg_slot):
    ents, width = table.shape
    slots = req_rows.shape[1]
    batch = head_slot.shape[0]
    vmem = pltpu.VMEM
    dma = pltpu.SemaphoreType.DMA
    scratch = [
        vmem((ents, width), BF16), vmem((4, relations.shape[0] // RELATION_PARTS, width), BF16), vmem((16, LANES), jnp.int32),
        vmem((1, LANES), jnp.int32), vmem((1, LANES), jnp.int32), vmem((24, LANES), jnp.int32),
        pltpu.SMEM((8, LANES), jnp.int32), vmem((1, slots), jnp.int32),
        vmem((16, LANES), F32), vmem((slots, LANES), F32), vmem((16, LANES), F32),
        vmem((3 * batch, LANES), F32), vmem(relations.shape, F32), vmem((24, LANES), F32),
        vmem((128, LANES), F32), vmem((16, LANES), F32), vmem((slots, width), BF16), vmem((slots, width), BF16),
        vmem((batch, width), F32), vmem((3 * batch, width), F32), vmem((batch, width), BF16),
        vmem((batch, width), BF16), vmem((batch, batch), BF16), vmem((3 * batch, width), BF16),
        vmem((slots, width), BF16), vmem((slots, width), BF16),
        dma((9,)), dma((4,)), dma, dma((GROUPS,)), dma, dma((GROUPS,)), dma, dma((GROUPS,)),
    ]
    return pl.pallas_call(
        kernel,
        out_shape=jax.ShapeDtypeStruct((ents, width), F32),
        in_specs=[pl.BlockSpec(memory_space=pltpu.HBM)] * 10,
        out_specs=pl.BlockSpec(memory_space=pltpu.VMEM),
        scratch_shapes=scratch,
        compiler_params=pltpu.CompilerParams(
            collective_id=0, has_side_effects=True, vmem_limit_bytes=50 * 2**20
        ),
        name="distmult_step",
    )(*[pltpu.with_memory_space_constraint(v, pltpu.HBM) for v in (
        table,
        relations,
        req_rows.reshape(16, LANES),
        owner_count,
        owner_start,
        head_slot.reshape(8, LANES),
        rel_id.reshape(8, LANES),
        tail_slot.reshape(8, LANES),
        neg_slot.reshape(8, LANES),
        jnp.asarray([[o[0] | o[1] << 2 | o[2] << 4 | o[3] << 6 for o in OFFSETS for _ in range(CAP)]], jnp.int32),
    )])


def solution(mesh):
    both = ("wide", "narrow")
    in_specs = (P(both, None), P(), P(both, None), P(both, None), P(both, None), P(both), P(both), P(both), P(both))
    return jax.shard_map(per_device, mesh=mesh, in_specs=in_specs, out_specs=P(both, None), check_vma=False)
```

```python
import jax
import jax.numpy as jnp
from jax import lax
from jax.experimental import pallas as pl
from jax.experimental.pallas import tpu as pltpu
from jax.sharding import PartitionSpec as P

MESH = pl.DeviceIdType.MESH
CAP = 16
SLOTS = 2048
RELATION_PARTS = 8
GROUP = 16
GROUPS = 8
SPAN = CAP * GROUP
LANES = 128
F32 = jnp.float32


def hops(offset):
    return sum(min(d, 4 - d) for d in offset[:3])


def partner_offsets():
    offsets = []
    for g in range(GROUPS):
        members = [(i // 4, i % 4, (g // 2 - i // 4 - i % 4) % 4, g % 2) for i in range(GROUP)]
        members.sort(key=lambda o: (o != (0, 0, 0, 0), -hops(o)))
        offsets += members
    return offsets


OFFSETS = partner_offsets()


def packed(digits):
    word = sum(d << (4 * i) for i, d in enumerate(digits))
    return word - (1 << 32) if word >= 1 << 31 else word


BF16 = jnp.bfloat16


def onehot(match):
    return jnp.where(match, 1.0, 0.0).astype(BF16)


def column(row):
    return jnp.transpose(jnp.broadcast_to(row, (LANES, LANES)))


def iota(shape, axis):
    return lax.broadcasted_iota(jnp.int32, shape, axis)


def kernel(
    table_h, rel_h, req_h, count_h, start_h, head_h, relid_h, tail_h, neg_h, offsets_h,
    out_ref,
    table, rel, req, count, start, look, relid, offsets,
    slotrow, slotcol, reqrow, lookcol, relwide, lookrow,
    idxbuf, wantrow, found, rows, rvec, emb, negb, perrow, sent, back,
    local_sem, rel_sem, id_send, id_recv, row_send, row_recv, grad_send, grad_recv,
):
    w = lax.axis_index("wide")
    y = lax.axis_index("narrow")
    x, z, core = w // 8, (w // 2) % 4, w % 2

    xs, zs = [((x + d) & 3) * 8 for d in range(4)], [((z + d) & 3) * 2 + core for d in range(4)]
    ys, cores = [(y + d) & 3 for d in range(4)], [0, 1 - 2 * core]

    def partner(n):
        dx, dz, dy, dc = OFFSETS[n]
        return (xs[dx] + zs[dz] + cores[dc], ys[dy])

    def each_partner(g, half, sign, act):
        for u in range(half * 8, half * 8 + 8):
            members = [OFFSETS[i * GROUP + u] for i in range(GROUPS)]
            xz = (packed([o[0] * 4 + o[1] for o in members]) >> (g * 4)) & 15
            yc = (packed([o[2] * 2 + o[3] for o in members]) >> (g * 4)) & 15
            px = (x + sign * (xz >> 2)) & 3
            pz = (z + sign * (xz & 3)) & 3
            py = (y + sign * (yc >> 1)) & 3
            device = (px * 8 + pz * 2 + ((core + yc) & 1), py)
            if u == 0:
                pl.when(g > 0)(lambda device=device: act(0, device))
            else:
                act(u, device)

    loads = [
        (start_h, start), (count_h, count), (req_h, req), (offsets_h, offsets), (table_h, table),
        (head_h, look.at[pl.ds(0, 8)]), (tail_h, look.at[pl.ds(8, 8)]), (neg_h, look.at[pl.ds(16, 8)]),
        (relid_h, relid),
    ]
    copies = [pltpu.make_async_copy(a, b, local_sem.at[i]) for i, (a, b) in enumerate(loads)]
    part = rel.shape[1]

    def load_relations(q):
        return pltpu.make_async_copy(
            rel_h.at[pl.ds(pl.multiple_of(q * part, part), part)], rel.at[q % 4], rel_sem.at[q % 4]
        )

    for copy in copies:
        copy.start()
    for q in range(4):
        load_relations(q).start()
    barrier = pltpu.get_barrier_semaphore()
    for n in sorted(range(1, GROUPS * GROUP), key=lambda n: -hops(OFFSETS[n])):
        pl.semaphore_signal(barrier, inc=1, device_id=partner(n), device_id_type=MESH)

    for copy in copies[:5]:
        copy.wait()

    row16 = iota((16, LANES), 0)
    first, many = start[...], count[...]
    facts = jnp.where(row16 == 0, first >> 6, jnp.where(row16 == 1, first & 63, jnp.where(row16 == 2, many, 0)))
    facts = facts.astype(F32).astype(BF16)
    asked = req[...]
    digits = jnp.concatenate([asked >> 5, asked & 31], axis=0).astype(F32).astype(BF16)
    lane = iota((1, SLOTS), 1)
    down = iota((LANES, SLOTS), 0)
    c = lane & 15
    off = offsets[...]
    ox, oz, oy, oc = off & 3, (off >> 2) & 3, (off >> 4) & 3, off >> 6
    owner = ((((x + ox) & 3) * 4 + ((z + oz) & 3)) * 2 + ((core + oc) & 1)) * 4 + ((y + oy) & 3)
    known = jnp.dot(facts, onehot(down == owner), preferred_element_type=F32)
    slot = (known[0:1] * 64.0 + known[1:2]).astype(jnp.int32) + c
    live = c < known[2:3].astype(jnp.int32)
    place = jnp.where(live, slot, -1).astype(F32)
    picked = jnp.dot(digits, onehot(down == (slot & 127)), preferred_element_type=F32)
    mine = iota((16, SLOTS), 0) == (slot >> 7)
    high = jnp.sum(jnp.where(mine, picked[:16], 0.0), axis=0, keepdims=True)
    low = jnp.sum(jnp.where(mine, picked[16:], 0.0), axis=0, keepdims=True)
    wanted = jnp.where(live, high * 32.0 + low, 0.0)
    for r in range(16):
        slotrow[r : r + 1] = place[:, r * LANES : (r + 1) * LANES]
        reqrow[r : r + 1] = wanted[:, r * LANES : (r + 1) * LANES]

    pl.semaphore_wait(barrier, GROUPS * GROUP - 1)

    for n in range(1, GROUPS * GROUP):
        pltpu.make_async_remote_copy(
            src_ref=reqrow.at[pl.ds(n // 8, 1)],
            dst_ref=idxbuf.at[pl.ds(n, 1)],
            send_sem=id_send,
            recv_sem=id_recv.at[n // 8],
            device_id=partner(n),
            device_id_type=MESH,
        ).start()

    idxbuf[0:1] = reqrow[0:1]

    some_device = partner(2)

    def arrived(buf, sem, g, blocks, unit):
        def wait(first, n):
            at = first * unit if isinstance(first, int) else pl.multiple_of(first * unit, unit)
            part = buf.at[pl.ds(at, n * unit)]
            pltpu.make_async_remote_copy(
                src_ref=part, dst_ref=part, send_sem=sem.at[g], recv_sem=sem.at[g],
                device_id=some_device, device_id_type=MESH,
            ).wait_recv()

        if isinstance(g, int):
            wait(g * blocks + (g == 0), blocks - (g == 0))
        else:
            pl.when(g == 0)(lambda: wait(1, blocks - 1))
            pl.when(g > 0)(lambda: wait(g * blocks, blocks))

    def drained(buf, sem, unit):
        n = GROUPS * GROUP - 1
        part = buf.at[pl.ds(unit, n * unit)]
        pltpu.make_async_remote_copy(
            src_ref=part, dst_ref=part, send_sem=sem, recv_sem=sem, device_id=some_device, device_id_type=MESH
        ).wait_send()

    def send_blocks(src, dst, send_sem, recv_sem, g, half, sign):
        def send(u, device):
            at = pl.ds(pl.multiple_of((g * GROUP + u) * CAP, CAP), CAP)
            pltpu.make_async_remote_copy(
                src_ref=src.at[at], dst_ref=dst.at[at], send_sem=send_sem, recv_sem=recv_sem.at[g * 2 + half],
                device_id=device, device_id_type=MESH,
            ).start()

        each_partner(g, half, sign, send)

    for copy in copies[5:9]:
        copy.wait()
    lookrow[...] = look[...].astype(F32)

    def columns(dst, src, n):
        @pl.loop(0, n // 8)
        def _(i):
            for e in range(8):
                at = pl.ds(pl.multiple_of((i * 8 + e) * LANES, LANES), LANES)
                dst[at] = column(src[pl.ds(i * 8 + e, 1)])

    columns(lookcol, lookrow, 24)
    columns(slotcol, slotrow, 16)

    def widen_relations(q):
        load_relations(q).wait()
        for e in range(4):
            rows_at = pl.ds(pl.multiple_of(q * part + e * (part // 4), 8), part // 4)
            relwide[rows_at] = rel[q % 4, pl.ds(e * (part // 4), part // 4)].astype(F32)

    @pl.loop(0, GROUPS)
    def _(g):
        belongs = (iota((8, LANES), 1) >> 4) == iota((8, LANES), 0)
        across = iota((LANES, LANES), 1)
        for half in range(2):
            arrived(idxbuf, id_recv, g * 2 + half, 8, 1)
            got = idxbuf[pl.ds(pl.multiple_of(g * 16 + half * 8, 8), 8)]
            row = jnp.sum(jnp.where(belongs, got, 0.0), axis=0, keepdims=True)
            wantrow[pl.ds(g * 2 + half, 1)] = row
            want = column(row).astype(jnp.int32)
            pick = jnp.concatenate([onehot(want == across + n * LANES) for n in range(8)], axis=1)
            here = jnp.dot(pick, table[...], preferred_element_type=F32).astype(BF16)
            found[pl.ds(pl.multiple_of(g * SPAN + half * LANES, LANES), LANES)] = here
            send_blocks(found, rows, row_send, row_recv, g, half, -1)

    rows[0:CAP] = found[0:CAP]

    @pl.loop(0, RELATION_PARTS)
    def _(q):
        widen_relations(q)
        pl.when(q + 4 < RELATION_PARTS)(lambda: load_relations(q + 4).start())

    @pl.loop(0, rvec.shape[0] // 32)
    def _(i):
        for e in range(32):
            row = relid[i // 4, (i % 4) * 32 + e]
            rvec[pl.ds(i * 32 + e, 1)] = relwide[pl.ds(row, 1)]

    emb[...] = jnp.zeros_like(emb)

    def gather_slots(first, halves):
        for h in range(halves):
            arrived(rows, row_recv, first + h, 8, CAP)

        @pl.loop(0, 3)
        def _(b):
            at = pl.ds(pl.multiple_of(b * 1024, 1024), 1024)
            ids = lookcol[at]
            places = [slotrow[pl.ds(first + h, 1)] for h in range(halves)]
            pick = jnp.concatenate([onehot(ids == place) for place in places], axis=1)
            span = rows[pl.ds(first * LANES, halves * LANES)]
            emb[at] += jnp.dot(pick, span, preferred_element_type=F32)

    for half, halves in ((0, 4), (4, 4), (8, 2), (10, 2), (12, 2), (14, 2)):
        gather_slots(half, halves)

    negb[...] = emb[2048:].astype(BF16)

    for b in range(2):
        at, tail_at = pl.ds(b * 512, 512), pl.ds(1024 + b * 512, 512)
        r = rvec[at]
        query = emb[at] * r
        half = query.astype(BF16)
        tail = emb[tail_at]
        positive = jnp.sum(query * tail, axis=1, keepdims=True)
        pos_weight = -1.0 / (1.0 + jnp.exp(positive))
        perrow[tail_at] = (pos_weight * query).astype(BF16)
        score = lax.dot_general(half, negb[...], (((1,), (1,)), ((), ())), preferred_element_type=F32)
        weight = (1.0 / (1.0 + jnp.exp(-score))).astype(BF16)
        pulled = jnp.dot(weight, negb[...], preferred_element_type=F32)
        perrow[at] = (r * (pos_weight * tail + pulled)).astype(BF16)
        pushed = lax.dot_general(weight, half, (((0,), (0,)), ((), ())), preferred_element_type=F32)
        if b == 0:
            emb[2048:] = pushed
        elif b < 1:
            emb[2048:] += pushed
        else:
            perrow[2048:] = (emb[2048:] + pushed).astype(BF16)

    @pl.loop(0, GROUPS)
    def _(i):
        g = GROUPS - 1 - i
        for half in range(2):
            at = pl.ds(pl.multiple_of(g * SPAN + half * LANES, LANES), LANES)
            place = slotcol[at]
            pick = jnp.concatenate([onehot(place == lookrow[n : n + 1]) for n in range(24)], axis=1)
            sent[at] = jnp.dot(pick, perrow[...], preferred_element_type=F32).astype(BF16)
            send_blocks(sent, back, grad_send, grad_recv, g, half, 1)

    back[0:CAP] = sent[0:CAP]
    out_ref[...] = jnp.zeros_like(out_ref)

    for i in range(2 * GROUPS):
        h = 2 * (GROUPS - 1 - i // 2) + i % 2
        arrived(back, grad_recv, h, 8, CAP)
        down = iota((1024, LANES), 0).astype(F32)
        pick = onehot(down == wantrow[h : h + 1])
        out_ref[...] += jnp.dot(pick, back[h * LANES : (h + 1) * LANES], preferred_element_type=F32)

    drained(idxbuf, id_send, 1)
    drained(found, row_send, CAP)
    drained(sent, grad_send, CAP)


def per_device(table, relations, req_rows, owner_count, owner_start, head_slot, rel_id, tail_slot, neg_slot):
    ents, width = table.shape
    slots = req_rows.shape[1]
    batch = head_slot.shape[0]
    vmem = pltpu.VMEM
    dma = pltpu.SemaphoreType.DMA
    scratch = [
        vmem((ents, width), BF16), vmem((4, relations.shape[0] // RELATION_PARTS, width), BF16), vmem((16, LANES), jnp.int32),
        vmem((1, LANES), jnp.int32), vmem((1, LANES), jnp.int32), vmem((24, LANES), jnp.int32),
        pltpu.SMEM((8, LANES), jnp.int32), vmem((1, slots), jnp.int32),
        vmem((16, LANES), F32), vmem((slots, LANES), F32), vmem((16, LANES), F32),
        vmem((3 * batch, LANES), F32), vmem(relations.shape, F32), vmem((24, LANES), F32),
        vmem((128, LANES), F32), vmem((16, LANES), F32), vmem((slots, width), BF16), vmem((slots, width), BF16),
        vmem((batch, width), F32), vmem((3 * batch, width), F32), vmem((batch, width), BF16),
        vmem((3 * batch, width), BF16),
        vmem((slots, width), BF16), vmem((slots, width), BF16),
        dma((9,)), dma((4,)), dma, dma((2 * GROUPS,)), dma, dma((2 * GROUPS,)), dma, dma((2 * GROUPS,)),
    ]
    return pl.pallas_call(
        kernel,
        out_shape=jax.ShapeDtypeStruct((ents, width), F32),
        in_specs=[pl.BlockSpec(memory_space=pltpu.HBM)] * 10,
        out_specs=pl.BlockSpec(memory_space=pltpu.VMEM),
        scratch_shapes=scratch,
        compiler_params=pltpu.CompilerParams(
            collective_id=0, has_side_effects=True, vmem_limit_bytes=50 * 2**20
        ),
        name="distmult_step",
    )(*[pltpu.with_memory_space_constraint(v, pltpu.HBM) for v in (
        table,
        relations,
        req_rows.reshape(16, LANES),
        owner_count,
        owner_start,
        head_slot.reshape(8, LANES),
        rel_id.reshape(8, LANES),
        tail_slot.reshape(8, LANES),
        neg_slot.reshape(8, LANES),
        jnp.asarray([[o[0] | o[1] << 2 | o[2] << 4 | o[3] << 6 for o in OFFSETS for _ in range(CAP)]], jnp.int32),
    )])


def solution(mesh):
    both = ("wide", "narrow")
    in_specs = (P(both, None), P(), P(both, None), P(both, None), P(both, None), P(both), P(both), P(both), P(both))
    return jax.shard_map(per_device, mesh=mesh, in_specs=in_specs, out_specs=P(both, None), check_vma=False)
```

```python
import jax
import jax.numpy as jnp
from jax import lax
from jax.experimental import pallas as pl
from jax.experimental.pallas import tpu as pltpu
from jax.sharding import PartitionSpec as P

MESH = pl.DeviceIdType.MESH
CAP = 16
SLOTS = 2048
RELATION_PARTS = 8
GROUP = 16
GROUPS = 8
SPAN = CAP * GROUP
LANES = 128
F32 = jnp.float32


def hops(offset):
    return sum(min(d, 4 - d) for d in offset[:3])


def partner_offsets():
    offsets = []
    for g in range(GROUPS):
        members = [(i // 4, i % 4, (g // 2 - i // 4 - i % 4) % 4, g % 2) for i in range(GROUP)]
        members.sort(key=lambda o: (o != (0, 0, 0, 0), -hops(o)))
        offsets += members
    return offsets


OFFSETS = partner_offsets()


def packed(digits):
    word = sum(d << (4 * i) for i, d in enumerate(digits))
    return word - (1 << 32) if word >= 1 << 31 else word


BF16 = jnp.bfloat16


def onehot(match):
    return jnp.where(match, 1.0, 0.0).astype(BF16)


def column(row):
    return jnp.transpose(jnp.broadcast_to(row, (LANES, LANES)))


def iota(shape, axis):
    return lax.broadcasted_iota(jnp.int32, shape, axis)


def kernel(
    table_h, rel_h, req_h, count_h, start_h, head_h, relid_h, tail_h, neg_h, offsets_h,
    out_ref,
    table, rel, req, count, start, look, relid, offsets,
    slotrow, slotcol, reqrow, lookcol, relwide, lookrow,
    idxbuf, wantrow, found, rows, rvec, emb, negb, perrow, sent, back,
    local_sem, rel_sem, id_send, id_recv, row_send, row_recv, grad_send, grad_recv,
):
    w = lax.axis_index("wide")
    y = lax.axis_index("narrow")
    x, z, core = w // 8, (w // 2) % 4, w % 2

    xs, zs = [((x + d) & 3) * 8 for d in range(4)], [((z + d) & 3) * 2 + core for d in range(4)]
    ys, cores = [(y + d) & 3 for d in range(4)], [0, 1 - 2 * core]

    def partner(n):
        dx, dz, dy, dc = OFFSETS[n]
        return (xs[dx] + zs[dz] + cores[dc], ys[dy])

    def each_partner(g, half, sign, act):
        for u in range(half * 8, half * 8 + 8):
            members = [OFFSETS[i * GROUP + u] for i in range(GROUPS)]
            xz = (packed([o[0] * 4 + o[1] for o in members]) >> (g * 4)) & 15
            yc = (packed([o[2] * 2 + o[3] for o in members]) >> (g * 4)) & 15
            px = (x + sign * (xz >> 2)) & 3
            pz = (z + sign * (xz & 3)) & 3
            py = (y + sign * (yc >> 1)) & 3
            device = (px * 8 + pz * 2 + ((core + yc) & 1), py)
            if u == 0:
                pl.when(g > 0)(lambda device=device: act(0, device))
            else:
                act(u, device)

    loads = [
        (start_h, start), (count_h, count), (req_h, req), (offsets_h, offsets), (table_h, table),
        (head_h, look.at[pl.ds(0, 8)]), (tail_h, look.at[pl.ds(8, 8)]), (neg_h, look.at[pl.ds(16, 8)]),
        (relid_h, relid),
    ]
    copies = [pltpu.make_async_copy(a, b, local_sem.at[i]) for i, (a, b) in enumerate(loads)]
    part = rel.shape[1]

    def load_relations(q):
        return pltpu.make_async_copy(
            rel_h.at[pl.ds(pl.multiple_of(q * part, part), part)], rel.at[q % 4], rel_sem.at[q % 4]
        )

    for copy in copies[:5]:
        copy.start()
    barrier = pltpu.get_barrier_semaphore()
    for n in sorted(range(1, GROUPS * GROUP), key=lambda n: -hops(OFFSETS[n])):
        pl.semaphore_signal(barrier, inc=1, device_id=partner(n), device_id_type=MESH)

    for copy in copies[5:]:
        copy.start()
    for q in range(4):
        load_relations(q).start()
    for copy in copies[:4]:
        copy.wait()

    row16 = iota((16, LANES), 0)
    first, many = start[...], count[...]
    facts = jnp.where(row16 == 0, first >> 6, jnp.where(row16 == 1, first & 63, jnp.where(row16 == 2, many, 0)))
    facts = facts.astype(F32).astype(BF16)
    asked = req[...]
    digits = jnp.concatenate([asked >> 5, asked & 31], axis=0).astype(F32).astype(BF16)
    lane = iota((1, SLOTS), 1)
    down = iota((LANES, SLOTS), 0)
    c = lane & 15
    off = offsets[...]
    ox, oz, oy, oc = off & 3, (off >> 2) & 3, (off >> 4) & 3, off >> 6
    owner = ((((x + ox) & 3) * 4 + ((z + oz) & 3)) * 2 + ((core + oc) & 1)) * 4 + ((y + oy) & 3)
    known = jnp.dot(facts, onehot(down == owner), preferred_element_type=F32)
    slot = (known[0:1] * 64.0 + known[1:2]).astype(jnp.int32) + c
    live = c < known[2:3].astype(jnp.int32)
    place = jnp.where(live, slot, -1).astype(F32)
    picked = jnp.dot(digits, onehot(down == (slot & 127)), preferred_element_type=F32)
    mine = iota((16, SLOTS), 0) == (slot >> 7)
    high = jnp.sum(jnp.where(mine, picked[:16], 0.0), axis=0, keepdims=True)
    low = jnp.sum(jnp.where(mine, picked[16:], 0.0), axis=0, keepdims=True)
    wanted = jnp.where(live, high * 32.0 + low, 0.0)
    for r in range(16):
        slotrow[r : r + 1] = place[:, r * LANES : (r + 1) * LANES]
        reqrow[r : r + 1] = wanted[:, r * LANES : (r + 1) * LANES]

    pl.semaphore_wait(barrier, GROUPS * GROUP - 1)

    for n in range(1, GROUPS * GROUP):
        pltpu.make_async_remote_copy(
            src_ref=reqrow.at[pl.ds(n // 8, 1)],
            dst_ref=idxbuf.at[pl.ds(n, 1)],
            send_sem=id_send,
            recv_sem=id_recv.at[n // 8],
            device_id=partner(n),
            device_id_type=MESH,
        ).start()

    idxbuf[0:1] = reqrow[0:1]

    some_device = partner(2)

    def arrived(buf, sem, g, blocks, unit):
        def wait(first, n):
            at = first * unit if isinstance(first, int) else pl.multiple_of(first * unit, unit)
            part = buf.at[pl.ds(at, n * unit)]
            pltpu.make_async_remote_copy(
                src_ref=part, dst_ref=part, send_sem=sem.at[g], recv_sem=sem.at[g],
                device_id=some_device, device_id_type=MESH,
            ).wait_recv()

        if isinstance(g, int):
            wait(g * blocks + (g == 0), blocks - (g == 0))
        else:
            pl.when(g == 0)(lambda: wait(1, blocks - 1))
            pl.when(g > 0)(lambda: wait(g * blocks, blocks))

    def drained(buf, sem, unit):
        n = GROUPS * GROUP - 1
        part = buf.at[pl.ds(unit, n * unit)]
        pltpu.make_async_remote_copy(
            src_ref=part, dst_ref=part, send_sem=sem, recv_sem=sem, device_id=some_device, device_id_type=MESH
        ).wait_send()

    def send_blocks(src, dst, send_sem, recv_sem, g, half, sign):
        def send(u, device):
            at = pl.ds(pl.multiple_of((g * GROUP + u) * CAP, CAP), CAP)
            pltpu.make_async_remote_copy(
                src_ref=src.at[at], dst_ref=dst.at[at], send_sem=send_sem, recv_sem=recv_sem.at[g * 2 + half],
                device_id=device, device_id_type=MESH,
            ).start()

        each_partner(g, half, sign, send)

    for copy in copies[4:9]:
        copy.wait()
    lookrow[...] = look[...].astype(F32)

    def columns(dst, src, n):
        @pl.loop(0, n // 8)
        def _(i):
            for e in range(8):
                at = pl.ds(pl.multiple_of((i * 8 + e) * LANES, LANES), LANES)
                dst[at] = column(src[pl.ds(i * 8 + e, 1)])

    columns(lookcol, lookrow, 24)
    columns(slotcol, slotrow, 16)

    def widen_relations(q):
        load_relations(q).wait()
        for e in range(4):
            rows_at = pl.ds(pl.multiple_of(q * part + e * (part // 4), 8), part // 4)
            relwide[rows_at] = rel[q % 4, pl.ds(e * (part // 4), part // 4)].astype(F32)

    @pl.loop(0, GROUPS)
    def _(g):
        belongs = (iota((8, LANES), 1) >> 4) == iota((8, LANES), 0)
        across = iota((LANES, LANES), 1)
        for half in range(2):
            arrived(idxbuf, id_recv, g * 2 + half, 8, 1)
            got = idxbuf[pl.ds(pl.multiple_of(g * 16 + half * 8, 8), 8)]
            row = jnp.sum(jnp.where(belongs, got, 0.0), axis=0, keepdims=True)
            wantrow[pl.ds(g * 2 + half, 1)] = row
            want = column(row).astype(jnp.int32)
            pick = jnp.concatenate([onehot(want == across + n * LANES) for n in range(8)], axis=1)
            here = jnp.dot(pick, table[...], preferred_element_type=F32).astype(BF16)
            found[pl.ds(pl.multiple_of(g * SPAN + half * LANES, LANES), LANES)] = here
            send_blocks(found, rows, row_send, row_recv, g, half, -1)

    rows[0:CAP] = found[0:CAP]

    @pl.loop(0, RELATION_PARTS)
    def _(q):
        widen_relations(q)
        pl.when(q + 4 < RELATION_PARTS)(lambda: load_relations(q + 4).start())

    @pl.loop(0, rvec.shape[0] // 32)
    def _(i):
        for e in range(32):
            row = relid[i // 4, (i % 4) * 32 + e]
            rvec[pl.ds(i * 32 + e, 1)] = relwide[pl.ds(row, 1)]

    emb[...] = jnp.zeros_like(emb)

    def gather_slots(first, halves):
        for h in range(halves):
            arrived(rows, row_recv, first + h, 8, CAP)

        def found_in(at):
            ids = lookcol[at]
            places = [slotrow[pl.ds(first + h, 1)] for h in range(halves)]
            pick = jnp.concatenate([onehot(ids == place) for place in places], axis=1)
            span = rows[pl.ds(first * LANES, halves * LANES)]
            return emb[at] + jnp.dot(pick, span, preferred_element_type=F32)

        last = first + halves == 2 * GROUPS

        @pl.loop(0, 2 if last else 3)
        def _(b):
            at = pl.ds(pl.multiple_of(b * 1024, 1024), 1024)
            emb[at] = found_in(at)

        if last:
            negb[...] = found_in(pl.ds(2048, 1024)).astype(BF16)

    for half, halves in ((0, 4), (4, 4), (8, 2), (10, 2), (12, 2), (14, 2)):
        gather_slots(half, halves)


    for b in range(2):
        at, tail_at = pl.ds(b * 512, 512), pl.ds(1024 + b * 512, 512)
        r = rvec[at]
        query = emb[at] * r
        half = query.astype(BF16)
        tail = emb[tail_at]
        positive = jnp.sum(query * tail, axis=1, keepdims=True)
        pos_weight = -1.0 / (1.0 + jnp.exp(positive))
        perrow[tail_at] = (pos_weight * query).astype(BF16)
        score = lax.dot_general(half, negb[...], (((1,), (1,)), ((), ())), preferred_element_type=F32)
        weight = (1.0 / (1.0 + jnp.exp(-score))).astype(BF16)
        pulled = jnp.dot(weight, negb[...], preferred_element_type=F32)
        perrow[at] = (r * (pos_weight * tail + pulled)).astype(BF16)
        pushed = lax.dot_general(weight, half, (((0,), (0,)), ((), ())), preferred_element_type=F32)
        if b == 0:
            emb[2048:] = pushed
        elif b < 1:
            emb[2048:] += pushed
        else:
            perrow[2048:] = (emb[2048:] + pushed).astype(BF16)

    @pl.loop(0, GROUPS)
    def _(i):
        g = GROUPS - 1 - i
        for half in range(2):
            at = pl.ds(pl.multiple_of(g * SPAN + half * LANES, LANES), LANES)
            place = slotcol[at]
            pick = jnp.concatenate([onehot(place == lookrow[n : n + 1]) for n in range(24)], axis=1)
            sent[at] = jnp.dot(pick, perrow[...], preferred_element_type=F32).astype(BF16)
            send_blocks(sent, back, grad_send, grad_recv, g, half, 1)

    back[0:CAP] = sent[0:CAP]
    out_ref[...] = jnp.zeros_like(out_ref)

    for i in range(2 * GROUPS):
        h = 2 * (GROUPS - 1 - i // 2) + i % 2
        arrived(back, grad_recv, h, 8, CAP)
        down = iota((1024, LANES), 0).astype(F32)
        pick = onehot(down == wantrow[h : h + 1])
        out_ref[...] += jnp.dot(pick, back[h * LANES : (h + 1) * LANES], preferred_element_type=F32)

    drained(idxbuf, id_send, 1)
    drained(found, row_send, CAP)
    drained(sent, grad_send, CAP)


def per_device(table, relations, req_rows, owner_count, owner_start, head_slot, rel_id, tail_slot, neg_slot):
    ents, width = table.shape
    slots = req_rows.shape[1]
    batch = head_slot.shape[0]
    vmem = pltpu.VMEM
    dma = pltpu.SemaphoreType.DMA
    scratch = [
        vmem((ents, width), BF16), vmem((4, relations.shape[0] // RELATION_PARTS, width), BF16), vmem((16, LANES), jnp.int32),
        vmem((1, LANES), jnp.int32), vmem((1, LANES), jnp.int32), vmem((24, LANES), jnp.int32),
        pltpu.SMEM((8, LANES), jnp.int32), vmem((1, slots), jnp.int32),
        vmem((16, LANES), F32), vmem((slots, LANES), F32), vmem((16, LANES), F32),
        vmem((3 * batch, LANES), F32), vmem(relations.shape, F32), vmem((24, LANES), F32),
        vmem((128, LANES), F32), vmem((16, LANES), F32), vmem((slots, width), BF16), vmem((slots, width), BF16),
        vmem((batch, width), F32), vmem((3 * batch, width), F32), vmem((batch, width), BF16),
        vmem((3 * batch, width), BF16),
        vmem((slots, width), BF16), vmem((slots, width), BF16),
        dma((9,)), dma((4,)), dma, dma((2 * GROUPS,)), dma, dma((2 * GROUPS,)), dma, dma((2 * GROUPS,)),
    ]
    return pl.pallas_call(
        kernel,
        out_shape=jax.ShapeDtypeStruct((ents, width), F32),
        in_specs=[pl.BlockSpec(memory_space=pltpu.HBM)] * 10,
        out_specs=pl.BlockSpec(memory_space=pltpu.VMEM),
        scratch_shapes=scratch,
        compiler_params=pltpu.CompilerParams(
            collective_id=0, has_side_effects=True, vmem_limit_bytes=50 * 2**20
        ),
        name="distmult_step",
    )(*[pltpu.with_memory_space_constraint(v, pltpu.HBM) for v in (
        table,
        relations,
        req_rows.reshape(16, LANES),
        owner_count,
        owner_start,
        head_slot.reshape(8, LANES),
        rel_id.reshape(8, LANES),
        tail_slot.reshape(8, LANES),
        neg_slot.reshape(8, LANES),
        jnp.asarray([[o[0] | o[1] << 2 | o[2] << 4 | o[3] << 6 for o in OFFSETS for _ in range(CAP)]], jnp.int32),
    )])


def solution(mesh):
    both = ("wide", "narrow")
    in_specs = (P(both, None), P(), P(both, None), P(both, None), P(both, None), P(both), P(both), P(both), P(both))
    return jax.shard_map(per_device, mesh=mesh, in_specs=in_specs, out_specs=P(both, None), check_vma=False)
```
